32 devices in a mesh: unit: 2 (over core), block: 4 (over z), lane: 4 (over y, x).
Axes of the slice: x: 2, y: 2, z: 4, core: 2. Of those that a mesh axis runs over, the one named last changes fastest.
Arguments:
- image_rows: bfloat16 [2048, 512], P(('unit', 'block', 'lane')), parts along dimension 0, may hold values from -6 to 6, as said below
- text_rows: bfloat16 [2048, 512], P(('unit', 'block', 'lane')), parts along dimension 0, may hold values from -6 to 6, as said below
Outputs:
- image_loss: float32 [2048], P(('unit', 'block', 'lane')), parts along dimension 0
- text_loss: float32 [2048], P(('unit', 'block', 'lane')), parts along dimension 0
- image_grad: float32 [2048, 512], P(('unit', 'block', 'lane')), parts along dimension 0
- text_grad: float32 [2048, 512], P(('unit', 'block', 'lane')), parts along dimension 0
The draws below stay inside these ranges and needn't reach their ends.
There are 2 independent parts, one for each index of `unit`. The reference program is written for one: setup_inputs(seed, part) draws one part's arguments, and reference() takes and returns one part's arrays. A program takes and returns all parts, laid end to end along the dimension named above; each array names one. Nothing has to cross between parts.
Inputs may be any that keep to these rules, and one draw needn't show every extreme that they name: image_rows holds numbers from -6 to 6. text_rows holds numbers from -6 to 6.
All inputs are finite; a program needn't handle non-finite values.
Results may differ from the reference program's by a relative error of at most 0.0035.
Values may be sent and summed in bfloat16 or wider, within the bound.
A program may use at most 64 MiB of HBM per device.

```python
import jax
import jax.numpy as jnp
from jax import lax

EX_DEV = 64
EXAMPLES = 1024
EMBED = 512
DEVICES = 16


def shared_part(key):
    return jax.random.normal(jax.random.fold_in(key, 3), (EXAMPLES, EMBED), jnp.float32)


def one_tower(key, tag):
    own = jax.random.normal(jax.random.fold_in(key, tag), (EXAMPLES, EMBED), jnp.float32)
    group = jax.random.normal(jax.random.fold_in(key, 4), (DEVICES, 1, EMBED), jnp.float32)
    values = 0.6 * shared_part(key) + own
    values = values.reshape(DEVICES, EX_DEV, EMBED) + 0.7 * group
    return jnp.clip(values, -6.0, 6.0).reshape(EXAMPLES, EMBED).astype(jnp.bfloat16)


def draw_image_rows(key, part):
    return one_tower(key, 1)


def draw_text_rows(key, part):
    return one_tower(key, 2)


def setup_inputs(seed: int = 0, part: int = 0) -> dict:
    arg_keys = jax.random.split(jax.random.key(seed), 3)
    part_keys = jax.random.split(jax.random.fold_in(arg_keys[2], part), 3)
    return {
        "image_rows": draw_image_rows(jax.random.fold_in(jax.random.fold_in(arg_keys[2], part), 71), part),
        "text_rows": draw_text_rows(jax.random.fold_in(jax.random.fold_in(arg_keys[2], part), 71), part),
    }


def unit_rows(values):
    wide = values.astype(jnp.float32)
    return (wide * lax.rsqrt(lax.optimization_barrier(jnp.sum(wide * wide, axis=-1, keepdims=True)) + 1e-06)).astype(jnp.bfloat16)

def reference(image_rows, text_rows):
    image_unit, text_unit = lax.optimization_barrier((unit_rows(image_rows), unit_rows(text_rows)))
    blocks = image_unit.reshape(DEVICES, EX_DEV, EMBED)

    def block_sums(column_sum, block):
        power = jnp.exp(12.0 * jnp.dot(block, text_unit.T, preferred_element_type=jnp.float32))
        return (column_sum + lax.optimization_barrier(jnp.sum(power, axis=0)), lax.optimization_barrier(jnp.sum(power, axis=1)))
    column_sum, row_sum = lax.scan(block_sums, jnp.zeros((EXAMPLES,), jnp.float32), blocks)
    row_sum = row_sum.reshape(EXAMPLES)
    matched = 12.0 * lax.optimization_barrier(jnp.sum(image_unit.astype(jnp.float32) * text_unit.astype(jnp.float32), axis=1))
    image_loss, text_loss = (jnp.log(row_sum) - matched, jnp.log(column_sum) - matched)

    def block_grads(text_grad, item):
        block, sums, number = item
        power = jnp.exp(12.0 * jnp.dot(block, text_unit.T, preferred_element_type=jnp.float32))
        same = (number * EX_DEV + jnp.arange(EX_DEV))[:, None] == jnp.arange(EXAMPLES)[None, :]
        pull = (power / sums[:, None] + power / column_sum[None, :] - jnp.where(same, 2.0, 0.0)).astype(jnp.bfloat16)
        pull = lax.optimization_barrier(pull)
        image_part = jnp.dot(pull, text_unit, preferred_element_type=jnp.float32)
        return (text_grad + jnp.dot(pull.T, block, preferred_element_type=jnp.float32), image_part)
    text_grad, image_grad = lax.scan(block_grads, jnp.zeros((EXAMPLES, EMBED), jnp.float32), (blocks, row_sum.reshape(DEVICES, EX_DEV), jnp.arange(DEVICES)))
    image_grad = image_grad.reshape(EXAMPLES, EMBED)
    return (image_loss, text_loss, image_grad, text_grad)
```

```python
import functools

import jax
import jax.numpy as jnp
from jax import lax
from jax.experimental import pallas as pl
from jax.experimental.pallas import tpu as pltpu
from jax.sharding import PartitionSpec as P

NT = (((1,), (1,)), ((), ()))


def unit_rows(values):
    wide = values.astype(jnp.float32)
    scale = lax.rsqrt(jnp.sum(wide * wide, axis=-1, keepdims=True) + 1e-06)
    return (wide * scale).astype(jnp.bfloat16)


def upright(row):
    return jnp.transpose(jnp.broadcast_to(row, (8, row.shape[1])))[:, :1]


def own_piece(row, pieces, mine):
    size = row.shape[1] // pieces
    return sum(
        jnp.where(mine == piece, row[:, piece * size : (piece + 1) * size], 0.0)
        for piece in range(pieces)
    )


def kernel(
    lanes,
    blocks,
    group,
    image_hbm,
    text_hbm,
    image_loss,
    text_loss,
    image_grad,
    text_grad,
    image_raw,
    text_raw,
    images,
    texts,
    power,
    power_t,
    row_mine,
    row_in,
    col_mine,
    col_in,
    image_acc,
    image_out,
    image_in,
    text_out,
    text_in,
    text_own,
    load_sem,
    send_image,
    recv_image,
    send_text,
    recv_text,
    send_row,
    recv_row,
    send_col,
    recv_col,
    send_ig,
    recv_ig,
    send_tg,
    recv_tg,
):
    lane, block = lax.axis_index("lane"), lax.axis_index("block")
    rows = image_raw.shape[0]
    images_n, texts_n = lanes * rows, blocks * rows
    groups = texts_n // group
    per_group = group // rows

    loads = [
        pltpu.make_async_copy(image_hbm, image_raw, load_sem.at[0]),
        pltpu.make_async_copy(text_hbm, text_raw, load_sem.at[1]),
    ]
    for load in loads:
        load.start()
    barrier = pltpu.get_barrier_semaphore()
    for k in range(1, blocks):
        pl.semaphore_signal(barrier, inc=1, device_id={"block": lax.rem(block + k, blocks)})
    for k in range(1, lanes):
        pl.semaphore_signal(barrier, inc=1, device_id={"lane": lax.rem(lane + k, lanes)})

    my_image = pl.ds(pl.multiple_of(lane * rows, rows), rows)
    my_text = pl.ds(pl.multiple_of(block * rows, rows), rows)
    loads[1].wait()
    texts[my_text, :] = unit_rows(text_raw[...])
    loads[0].wait()
    images[my_image, :] = unit_rows(image_raw[...])
    pl.semaphore_wait(barrier, lanes + blocks - 2)

    def to_block(k, src, dst, send, recv):
        return pltpu.make_async_remote_copy(
            src_ref=src,
            dst_ref=dst,
            send_sem=send.at[k - 1],
            recv_sem=recv.at[k - 1],
            device_id={"block": lax.rem(block + k, blocks)},
        )

    def to_lane(k, src, dst, send, recv):
        return pltpu.make_async_remote_copy(
            src_ref=src,
            dst_ref=dst,
            send_sem=send.at[k - 1],
            recv_sem=recv.at[k - 1],
            device_id={"lane": lax.rem(lane + k, lanes)},
        )

    text_copies = [
        to_block(k, texts.at[my_text], texts.at[my_text], send_text, recv_text)
        for k in range(1, blocks)
    ]
    image_copies = [
        to_lane(k, images.at[my_image], images.at[my_image], send_image, recv_image)
        for k in range(1, lanes)
    ]
    for copy in text_copies + image_copies:
        copy.start()

    pair = 12.0 * lax.dot_general(
        images[my_image, :], texts[my_text, :], NT, preferred_element_type=jnp.float32
    )
    eye = lax.broadcasted_iota(jnp.int32, (rows, rows), 0) == lax.broadcasted_iota(
        jnp.int32, (rows, rows), 1
    )
    matched = jnp.sum(jnp.where(eye, pair, 0.0), axis=0, keepdims=True)

    for copy in image_copies + text_copies:
        copy.wait_recv()

    def over_groups(step, start):
        if groups == 1:
            return step(0, start)
        return lax.fori_loop(0, groups, step, start)

    def group_rows(g):
        return pl.ds(g * group if groups == 1 else pl.multiple_of(g * group, group), group)

    def power_step(g, row_sum):
        some = texts[group_rows(g), :]
        p = jnp.exp(12.0 * lax.dot_general(images[...], some, NT, preferred_element_type=jnp.float32))
        q = jnp.exp(12.0 * lax.dot_general(some, images[...], NT, preferred_element_type=jnp.float32))
        power[g] = p
        power_t[g] = q
        col_mine[g] = jnp.sum(p, axis=0, keepdims=True)
        return row_sum + jnp.sum(q, axis=0, keepdims=True)

    row_mine[...] = over_groups(power_step, jnp.zeros((1, images_n), jnp.float32))
    sum_copies = [
        to_block(k, col_mine, col_in.at[k - 1], send_col, recv_col) for k in range(1, blocks)
    ] + [to_lane(k, row_mine, row_in.at[k - 1], send_row, recv_row) for k in range(1, lanes)]
    for copy in sum_copies:
        copy.start()
    for copy in sum_copies:
        copy.wait_recv()

    row_sum = row_mine[...]
    for k in range(1, lanes):
        row_sum = row_sum + row_in[k - 1]
    row_inv = 1.0 / row_sum
    row_inv_up = upright(row_inv)
    image_loss[...] = jnp.log(own_piece(row_sum, lanes, lane)) - matched

    def col_total(g):
        total = col_mine[g]
        for k in range(1, blocks):
            total = total + col_in[k - 1, g]
        return total

    image_acc[...] = jnp.zeros_like(image_acc)

    def grad_step(g, own_col):
        total = col_total(g)
        col_inv = 1.0 / total
        col_inv_up = upright(col_inv)
        first = block - g * per_group
        ids_t = lax.broadcasted_iota(jnp.int32, (group, images_n), 0) - first * rows
        ids_i = lax.broadcasted_iota(jnp.int32, (group, images_n), 1) - lane * rows
        same_t = (ids_t == ids_i) & (ids_i >= 0) & (ids_i < rows)
        pull_t = (power_t[g] * (row_inv + col_inv_up) - jnp.where(same_t, 2.0, 0.0)).astype(
            jnp.bfloat16
        )
        part = jnp.dot(pull_t, images[...], preferred_element_type=jnp.float32)
        text_own[group_rows(g), :] = part
        text_out[group_rows(g), :] = part.astype(jnp.bfloat16)
        ids_i = lax.broadcasted_iota(jnp.int32, (images_n, group), 0) - lane * rows
        ids_t = lax.broadcasted_iota(jnp.int32, (images_n, group), 1) - first * rows
        same = (ids_t == ids_i) & (ids_i >= 0) & (ids_i < rows)
        pull = (power[g] * (row_inv_up + col_inv) - jnp.where(same, 2.0, 0.0)).astype(jnp.bfloat16)
        image_acc[...] += jnp.dot(
            pull, texts[group_rows(g), :], preferred_element_type=jnp.float32
        )
        return own_col + own_piece(total, per_group, first)

    own_col = over_groups(grad_step, jnp.zeros((1, rows), jnp.float32))
    image_out[...] = image_acc[...].astype(jnp.bfloat16)

    def there(index, count, k):
        return pl.ds(pl.multiple_of(lax.rem(index + k, count) * rows, rows), rows)

    tg_copies = [
        to_block(k, text_out.at[there(block, blocks, k)], text_in.at[k - 1], send_tg, recv_tg)
        for k in range(1, blocks)
    ]
    ig_copies = [
        to_lane(k, image_out.at[there(lane, lanes, k)], image_in.at[k - 1], send_ig, recv_ig)
        for k in range(1, lanes)
    ]
    for copy in tg_copies + ig_copies:
        copy.start()
    text_loss[...] = jnp.log(own_col) - matched
    for copy in ig_copies:
        copy.wait_recv()
    grad = image_acc[my_image, :]
    for k in range(1, lanes):
        grad = grad + image_in[k - 1].astype(jnp.float32)
    image_grad[...] = grad
    for copy in tg_copies:
        copy.wait_recv()
    grad = text_own[my_text, :]
    for k in range(1, blocks):
        grad = grad + text_in[k - 1].astype(jnp.float32)
    text_grad[...] = grad
    for copy in text_copies + image_copies + sum_copies + tg_copies + ig_copies:
        copy.wait_send()


def solution(mesh):
    lanes, blocks = mesh.shape["lane"], mesh.shape["block"]

    def body(image_rows, text_rows):
        rows, width = image_rows.shape
        images_n, texts_n = lanes * rows, blocks * rows
        group = rows * next(c for c in (4, 2, 1) if blocks % c == 0)
        groups = texts_n // group
        f32, bf16 = jnp.float32, jnp.bfloat16
        sems = [pltpu.SemaphoreType.DMA((2,))]
        for count in (lanes, blocks, lanes, blocks, lanes, blocks):
            sems += [pltpu.SemaphoreType.DMA((max(count - 1, 1),))] * 2
        image_loss, text_loss, image_grad, text_grad = pl.pallas_call(
            functools.partial(kernel, lanes, blocks, group),
            out_shape=(
                jax.ShapeDtypeStruct((1, rows), f32),
                jax.ShapeDtypeStruct((1, rows), f32),
                jax.ShapeDtypeStruct((rows, width), f32),
                jax.ShapeDtypeStruct((rows, width), f32),
            ),
            in_specs=[pl.BlockSpec(memory_space=pl.ANY)] * 2,
            out_specs=[pl.BlockSpec(memory_space=pltpu.VMEM)] * 4,
            scratch_shapes=[
                pltpu.VMEM((rows, width), bf16),
                pltpu.VMEM((rows, width), bf16),
                pltpu.VMEM((images_n, width), bf16),
                pltpu.VMEM((texts_n, width), bf16),
                pltpu.VMEM((groups, images_n, group), f32),
                pltpu.VMEM((groups, group, images_n), f32),
                pltpu.VMEM((1, images_n), f32),
                pltpu.VMEM((max(lanes - 1, 1), 1, images_n), f32),
                pltpu.VMEM((groups, 1, group), f32),
                pltpu.VMEM((max(blocks - 1, 1), groups, 1, group), f32),
                pltpu.VMEM((images_n, width), f32),
                pltpu.VMEM((images_n, width), bf16),
                pltpu.VMEM((max(lanes - 1, 1), rows, width), bf16),
                pltpu.VMEM((texts_n, width), bf16),
                pltpu.VMEM((max(blocks - 1, 1), rows, width), bf16),
                pltpu.VMEM((texts_n, width), f32),
            ]
            + sems,
            compiler_params=pltpu.CompilerParams(collective_id=0, has_side_effects=True),
        )(image_rows, text_rows)
        return (image_loss.reshape(rows), text_loss.reshape(rows), image_grad, text_grad)

    rows_spec = P(("unit", "block", "lane"), None)
    flat_spec = P(("unit", "block", "lane"))
    return jax.shard_map(
        body,
        mesh=mesh,
        in_specs=(rows_spec, rows_spec),
        out_specs=(flat_spec, flat_spec, rows_spec, rows_spec),
        check_vma=False,
    )
```

```python
import functools

import jax
import jax.numpy as jnp
from jax import lax
from jax.experimental import pallas as pl
from jax.experimental.pallas import tpu as pltpu
from jax.sharding import PartitionSpec as P

NT = (((1,), (1,)), ((), ()))


def unit_rows(values):
    wide = values.astype(jnp.float32)
    scale = lax.rsqrt(jnp.sum(wide * wide, axis=-1, keepdims=True) + 1e-06)
    return (wide * scale).astype(jnp.bfloat16)


def upright(row):
    return jnp.transpose(jnp.broadcast_to(row, (8, row.shape[1])))[:, :1]


def own_piece(row, pieces, mine):
    size = row.shape[1] // pieces
    return sum(
        jnp.where(mine == piece, row[:, piece * size : (piece + 1) * size], 0.0)
        for piece in range(pieces)
    )


def kernel(
    lanes,
    blocks,
    group,
    image_hbm,
    text_hbm,
    image_loss,
    text_loss,
    image_grad,
    text_grad,
    image_raw,
    text_raw,
    images,
    texts,
    power,
    power_t,
    row_mine,
    row_in,
    col_mine,
    col_in,
    image_acc,
    image_out,
    image_in,
    text_out,
    text_in,
    text_own,
    load_sem,
    send_image,
    recv_image,
    send_text,
    recv_text,
    send_row,
    recv_row,
    send_col,
    recv_col,
    send_ig,
    recv_ig,
    send_tg,
    recv_tg,
):
    lane, block = lax.axis_index("lane"), lax.axis_index("block")
    rows = image_raw.shape[0]
    images_n, texts_n = lanes * rows, blocks * rows
    groups = texts_n // group
    per_group = group // rows

    loads = [
        pltpu.make_async_copy(image_hbm, image_raw, load_sem.at[0]),
        pltpu.make_async_copy(text_hbm, text_raw, load_sem.at[1]),
    ]
    for load in loads:
        load.start()
    barrier = pltpu.get_barrier_semaphore()
    for k in range(1, blocks):
        pl.semaphore_signal(barrier, inc=1, device_id={"block": lax.rem(block + k, blocks)})
    for k in range(1, lanes):
        pl.semaphore_signal(barrier, inc=1, device_id={"lane": lax.rem(lane + k, lanes)})

    my_image = pl.ds(pl.multiple_of(lane * rows, rows), rows)
    my_text = pl.ds(pl.multiple_of(block * rows, rows), rows)
    loads[1].wait()
    texts[my_text, :] = unit_rows(text_raw[...])
    loads[0].wait()
    images[my_image, :] = unit_rows(image_raw[...])
    pl.semaphore_wait(barrier, lanes + blocks - 2)

    def to_block(k, src, dst, send, recv):
        return pltpu.make_async_remote_copy(
            src_ref=src,
            dst_ref=dst,
            send_sem=send.at[k - 1],
            recv_sem=recv.at[k - 1],
            device_id={"block": lax.rem(block + k, blocks)},
        )

    def to_lane(k, src, dst, send, recv):
        return pltpu.make_async_remote_copy(
            src_ref=src,
            dst_ref=dst,
            send_sem=send.at[k - 1],
            recv_sem=recv.at[k - 1],
            device_id={"lane": lax.rem(lane + k, lanes)},
        )

    text_copies = [
        to_block(k, texts.at[my_text], texts.at[my_text], send_text, recv_text)
        for k in range(1, blocks)
    ]
    image_copies = [
        to_lane(k, images.at[my_image], images.at[my_image], send_image, recv_image)
        for k in range(1, lanes)
    ]
    for copy in text_copies + image_copies:
        copy.start()

    pair = 12.0 * lax.dot_general(
        images[my_image, :], texts[my_text, :], NT, preferred_element_type=jnp.float32
    )
    eye = lax.broadcasted_iota(jnp.int32, (rows, rows), 0) == lax.broadcasted_iota(
        jnp.int32, (rows, rows), 1
    )
    matched = jnp.sum(jnp.where(eye, pair, 0.0), axis=0, keepdims=True)

    for copy in image_copies + text_copies:
        copy.wait_recv()

    def over_groups(step, start):
        if groups == 1:
            return step(0, start)
        return lax.fori_loop(0, groups, step, start)

    def group_rows(g):
        return pl.ds(g * group if groups == 1 else pl.multiple_of(g * group, group), group)

    def power_step(g, row_sum):
        some = texts[group_rows(g), :]
        p = jnp.exp(12.0 * lax.dot_general(images[...], some, NT, preferred_element_type=jnp.float32))
        q = jnp.exp(12.0 * lax.dot_general(some, images[...], NT, preferred_element_type=jnp.float32))
        power[g] = p
        power_t[g] = q
        col_mine[g] = jnp.sum(p, axis=0, keepdims=True)
        return row_sum + jnp.sum(q, axis=0, keepdims=True)

    row_mine[...] = over_groups(power_step, jnp.zeros((1, images_n), jnp.float32))
    sum_copies = [
        to_block(k, col_mine, col_in.at[k - 1], send_col, recv_col) for k in range(1, blocks)
    ] + [to_lane(k, row_mine, row_in.at[k - 1], send_row, recv_row) for k in range(1, lanes)]
    for copy in sum_copies:
        copy.start()
    for copy in sum_copies:
        copy.wait_recv()

    row_sum = row_mine[...]
    for k in range(1, lanes):
        row_sum = row_sum + row_in[k - 1]
    row_inv = 1.0 / row_sum
    row_inv_up = upright(row_inv)
    image_loss[...] = jnp.log(own_piece(row_sum, lanes, lane)) - matched

    def col_total(g):
        total = col_mine[g]
        for k in range(1, blocks):
            total = total + col_in[k - 1, g]
        return total

    image_acc[...] = jnp.zeros_like(image_acc)

    def grad_step(g, own_col):
        total = col_total(g)
        col_inv = 1.0 / total
        col_inv_up = upright(col_inv)
        first = block - g * per_group
        ids_t = lax.broadcasted_iota(jnp.int32, (group, images_n), 0) - first * rows
        ids_i = lax.broadcasted_iota(jnp.int32, (group, images_n), 1) - lane * rows
        same_t = (ids_t == ids_i) & (ids_i >= 0) & (ids_i < rows)
        pull_t = (power_t[g] * (row_inv + col_inv_up) - jnp.where(same_t, 2.0, 0.0)).astype(
            jnp.bfloat16
        )
        part = jnp.dot(pull_t, images[...], preferred_element_type=jnp.float32)
        text_own[group_rows(g), :] = part
        text_out[group_rows(g), :] = part.astype(jnp.bfloat16)
        ids_i = lax.broadcasted_iota(jnp.int32, (images_n, group), 0) - lane * rows
        ids_t = lax.broadcasted_iota(jnp.int32, (images_n, group), 1) - first * rows
        same = (ids_t == ids_i) & (ids_i >= 0) & (ids_i < rows)
        pull = (power[g] * (row_inv_up + col_inv) - jnp.where(same, 2.0, 0.0)).astype(jnp.bfloat16)
        image_acc[...] += jnp.dot(
            pull, texts[group_rows(g), :], preferred_element_type=jnp.float32
        )
        return own_col + own_piece(total, per_group, first)

    own_col = over_groups(grad_step, jnp.zeros((1, rows), jnp.float32))
    image_out[...] = image_acc[...].astype(jnp.bfloat16)

    def there(index, count, k):
        return pl.ds(pl.multiple_of(lax.rem(index + k, count) * rows, rows), rows)

    tg_copies = [
        to_block(k, text_out.at[there(block, blocks, k)], text_in.at[k - 1], send_tg, recv_tg)
        for k in range(1, blocks)
    ]
    ig_copies = [
        to_lane(k, image_out.at[there(lane, lanes, k)], image_in.at[k - 1], send_ig, recv_ig)
        for k in range(1, lanes)
    ]
    for copy in tg_copies + ig_copies:
        copy.start()
    text_loss[...] = jnp.log(own_col) - matched
    for copy in ig_copies:
        copy.wait_recv()
    grad = image_acc[my_image, :]
    for k in range(1, lanes):
        grad = grad + image_in[k - 1].astype(jnp.float32)
    image_grad[...] = grad
    for copy in tg_copies:
        copy.wait_recv()
    grad = text_own[my_text, :]
    for k in range(1, blocks):
        grad = grad + text_in[k - 1].astype(jnp.float32)
    text_grad[...] = grad
    for copy in text_copies + image_copies + sum_copies + tg_copies + ig_copies:
        copy.wait_send()


def place(*refs):
    sem = refs[-1]
    copies = [
        pltpu.make_async_copy(refs[i], refs[i + 4], sem.at[i]) for i in (2, 3, 0, 1)
    ]
    for copy in copies:
        copy.start()
    for copy in copies:
        copy.wait()


def solution(mesh):
    lanes, blocks = mesh.shape["lane"], mesh.shape["block"]

    def body(image_rows, text_rows):
        rows, width = image_rows.shape
        images_n, texts_n = lanes * rows, blocks * rows
        group = rows * next(c for c in (4, 2, 1) if blocks % c == 0)
        groups = texts_n // group
        f32, bf16 = jnp.float32, jnp.bfloat16
        limit = 4 * (
            images_n * texts_n * 8 + (images_n + texts_n) * width * 6 + rows * width * 64
        )
        limit = min(limit, 60 * 2**20)
        sems = [pltpu.SemaphoreType.DMA((2,))]
        for count in (lanes, blocks, lanes, blocks, lanes, blocks):
            sems += [pltpu.SemaphoreType.DMA((max(count - 1, 1),))] * 2
        image_loss, text_loss, image_grad, text_grad = pl.pallas_call(
            functools.partial(kernel, lanes, blocks, group),
            out_shape=(
                jax.ShapeDtypeStruct((1, rows), f32),
                jax.ShapeDtypeStruct((1, rows), f32),
                jax.ShapeDtypeStruct((rows, width), f32),
                jax.ShapeDtypeStruct((rows, width), f32),
            ),
            in_specs=[pl.BlockSpec(memory_space=pltpu.HBM)] * 2,
            out_specs=[pl.BlockSpec(memory_space=pltpu.VMEM)] * 4,
            scratch_shapes=[
                pltpu.VMEM((rows, width), bf16),
                pltpu.VMEM((rows, width), bf16),
                pltpu.VMEM((images_n, width), bf16),
                pltpu.VMEM((texts_n, width), bf16),
                pltpu.VMEM((groups, images_n, group), f32),
                pltpu.VMEM((groups, group, images_n), f32),
                pltpu.VMEM((1, images_n), f32),
                pltpu.VMEM((max(lanes - 1, 1), 1, images_n), f32),
                pltpu.VMEM((groups, 1, group), f32),
                pltpu.VMEM((max(blocks - 1, 1), groups, 1, group), f32),
                pltpu.VMEM((images_n, width), f32),
                pltpu.VMEM((images_n, width), bf16),
                pltpu.VMEM((max(lanes - 1, 1), rows, width), bf16),
                pltpu.VMEM((texts_n, width), bf16),
                pltpu.VMEM((max(blocks - 1, 1), rows, width), bf16),
                pltpu.VMEM((texts_n, width), f32),
            ]
            + sems,
            compiler_params=pltpu.CompilerParams(
                collective_id=0, has_side_effects=True, vmem_limit_bytes=limit
            ),
        )(image_rows, text_rows)
        results = (image_loss, text_loss, image_grad, text_grad)
        image_loss, text_loss, image_grad, text_grad = pl.pallas_call(
            place,
            out_shape=tuple(jax.ShapeDtypeStruct(r.shape, r.dtype) for r in results),
            in_specs=[pl.BlockSpec(memory_space=pltpu.VMEM)] * 4,
            out_specs=[pl.BlockSpec(memory_space=pl.ANY)] * 4,
            scratch_shapes=[pltpu.SemaphoreType.DMA((4,))],
            compiler_params=pltpu.CompilerParams(vmem_limit_bytes=4 * rows * width * 8),
        )(*results)
        return (image_loss.reshape(rows), text_loss.reshape(rows), image_grad, text_grad)

    rows_spec = P(("unit", "block", "lane"), None)
    flat_spec = P(("unit", "block", "lane"))
    return jax.shard_map(
        body,
        mesh=mesh,
        in_specs=(rows_spec, rows_spec),
        out_specs=(flat_spec, flat_spec, rows_spec, rows_spec),
        check_vma=False,
    )
```

```python
import functools

import jax
import jax.numpy as jnp
from jax import lax
from jax.experimental import pallas as pl
from jax.experimental.pallas import tpu as pltpu
from jax.sharding import PartitionSpec as P

NT = (((1,), (1,)), ((), ()))


def unit_rows(values):
    wide = values.astype(jnp.float32)
    scale = lax.rsqrt(jnp.sum(wide * wide, axis=-1, keepdims=True) + 1e-06)
    return (wide * scale).astype(jnp.bfloat16)


def upright(row):
    return jnp.transpose(jnp.broadcast_to(row, (8, row.shape[1])))[:, :1]


def own_piece(row, pieces, mine):
    size = row.shape[1] // pieces
    return sum(
        jnp.where(mine == piece, row[:, piece * size : (piece + 1) * size], 0.0)
        for piece in range(pieces)
    )


def kernel(
    lanes,
    blocks,
    group,
    image_hbm,
    text_hbm,
    image_loss,
    text_loss,
    image_grad,
    text_grad,
    image_raw,
    text_raw,
    images,
    texts,
    power,
    power_t,
    row_mine,
    row_in,
    col_mine,
    col_in,
    image_acc,
    image_out,
    image_in,
    text_out,
    text_in,
    text_own,
    load_sem,
    send_image,
    recv_image,
    send_text,
    recv_text,
    send_row,
    recv_row,
    send_col,
    recv_col,
    send_ig,
    recv_ig,
    send_tg,
    recv_tg,
):
    lane, block = lax.axis_index("lane"), lax.axis_index("block")
    rows = image_raw.shape[0]
    images_n, texts_n = lanes * rows, blocks * rows
    groups = texts_n // group
    per_group = group // rows

    loads = [
        pltpu.make_async_copy(image_hbm, image_raw, load_sem.at[0]),
        pltpu.make_async_copy(text_hbm, text_raw, load_sem.at[1]),
    ]
    for load in loads:
        load.start()
    barrier = pltpu.get_barrier_semaphore()
    for k in range(1, blocks):
        pl.semaphore_signal(barrier, inc=1, device_id={"block": lax.rem(block + k, blocks)})
    for k in range(1, lanes):
        pl.semaphore_signal(barrier, inc=1, device_id={"lane": lax.rem(lane + k, lanes)})

    my_image = pl.ds(pl.multiple_of(lane * rows, rows), rows)
    my_text = pl.ds(pl.multiple_of(block * rows, rows), rows)
    loads[1].wait()
    texts[my_text, :] = unit_rows(text_raw[...])
    loads[0].wait()
    images[my_image, :] = unit_rows(image_raw[...])
    pl.semaphore_wait(barrier, lanes + blocks - 2)

    def to_block(k, src, dst, send, recv):
        return pltpu.make_async_remote_copy(
            src_ref=src,
            dst_ref=dst,
            send_sem=send.at[k - 1],
            recv_sem=recv.at[k - 1],
            device_id={"block": lax.rem(block + k, blocks)},
        )

    def to_lane(k, src, dst, send, recv):
        return pltpu.make_async_remote_copy(
            src_ref=src,
            dst_ref=dst,
            send_sem=send.at[k - 1],
            recv_sem=recv.at[k - 1],
            device_id={"lane": lax.rem(lane + k, lanes)},
        )

    text_copies = [
        to_block(k, texts.at[my_text], texts.at[my_text], send_text, recv_text)
        for k in range(1, blocks)
    ]
    image_copies = [
        to_lane(k, images.at[my_image], images.at[my_image], send_image, recv_image)
        for k in range(1, lanes)
    ]
    for copy in text_copies + image_copies:
        copy.start()

    pair = 12.0 * lax.dot_general(
        images[my_image, :], texts[my_text, :], NT, preferred_element_type=jnp.float32
    )
    eye = lax.broadcasted_iota(jnp.int32, (rows, rows), 0) == lax.broadcasted_iota(
        jnp.int32, (rows, rows), 1
    )
    matched = jnp.sum(jnp.where(eye, pair, 0.0), axis=0, keepdims=True)

    for copy in image_copies + text_copies:
        copy.wait_recv()

    def over_groups(step, start):
        if groups == 1:
            return step(0, start)
        return lax.fori_loop(0, groups, step, start)

    def group_rows(g):
        return pl.ds(g * group if groups == 1 else pl.multiple_of(g * group, group), group)

    def power_step(g, row_sum):
        some = texts[group_rows(g), :]
        p = jnp.exp(12.0 * lax.dot_general(images[...], some, NT, preferred_element_type=jnp.float32))
        q = jnp.exp(12.0 * lax.dot_general(some, images[...], NT, preferred_element_type=jnp.float32))
        power[g] = p
        power_t[g] = q
        col_mine[g] = jnp.sum(p, axis=0, keepdims=True)
        return row_sum + jnp.sum(q, axis=0, keepdims=True)

    row_mine[...] = over_groups(power_step, jnp.zeros((1, images_n), jnp.float32))
    sum_copies = [
        to_block(k, col_mine, col_in.at[k - 1], send_col, recv_col) for k in range(1, blocks)
    ] + [to_lane(k, row_mine, row_in.at[k - 1], send_row, recv_row) for k in range(1, lanes)]
    for copy in sum_copies:
        copy.start()
    for copy in sum_copies:
        copy.wait_recv()

    row_sum = row_mine[...]
    for k in range(1, lanes):
        row_sum = row_sum + row_in[k - 1]
    row_inv = 1.0 / row_sum
    row_inv_up = upright(row_inv)
    image_loss[...] = jnp.log(own_piece(row_sum, lanes, lane)) - matched

    def col_total(g):
        total = col_mine[g]
        for k in range(1, blocks):
            total = total + col_in[k - 1, g]
        return total

    image_acc[...] = jnp.zeros_like(image_acc)

    def grad_step(g, own_col):
        total = col_total(g)
        col_inv = 1.0 / total
        col_inv_up = upright(col_inv)
        first = block - g * per_group
        ids_t = lax.broadcasted_iota(jnp.int32, (group, images_n), 0) - first * rows
        ids_i = lax.broadcasted_iota(jnp.int32, (group, images_n), 1) - lane * rows
        same_t = (ids_t == ids_i) & (ids_i >= 0) & (ids_i < rows)
        pull_t = (power_t[g] * (row_inv + col_inv_up) - jnp.where(same_t, 2.0, 0.0)).astype(
            jnp.bfloat16
        )
        part = jnp.dot(pull_t, images[...], preferred_element_type=jnp.float32)
        text_own[group_rows(g), :] = part
        text_out[group_rows(g), :] = part.astype(jnp.bfloat16)
        ids_i = lax.broadcasted_iota(jnp.int32, (images_n, group), 0) - lane * rows
        ids_t = lax.broadcasted_iota(jnp.int32, (images_n, group), 1) - first * rows
        same = (ids_t == ids_i) & (ids_i >= 0) & (ids_i < rows)
        pull = (power[g] * (row_inv_up + col_inv) - jnp.where(same, 2.0, 0.0)).astype(jnp.bfloat16)
        image_acc[...] += jnp.dot(
            pull, texts[group_rows(g), :], preferred_element_type=jnp.float32
        )
        return own_col + own_piece(total, per_group, first)

    own_col = over_groups(grad_step, jnp.zeros((1, rows), jnp.float32))
    image_out[...] = image_acc[...].astype(jnp.bfloat16)

    def there(index, count, k):
        return pl.ds(pl.multiple_of(lax.rem(index + k, count) * rows, rows), rows)

    tg_copies = [
        to_block(k, text_out.at[there(block, blocks, k)], text_in.at[k - 1], send_tg, recv_tg)
        for k in range(1, blocks)
    ]
    ig_copies = [
        to_lane(k, image_out.at[there(lane, lanes, k)], image_in.at[k - 1], send_ig, recv_ig)
        for k in range(1, lanes)
    ]
    for copy in tg_copies + ig_copies:
        copy.start()
    text_loss[...] = jnp.log(own_col) - matched
    for copy in ig_copies:
        copy.wait_recv()
    grad = image_acc[my_image, :]
    for k in range(1, lanes):
        grad = grad + image_in[k - 1].astype(jnp.float32)
    image_grad[...] = grad
    for copy in tg_copies:
        copy.wait_recv()
    grad = text_own[my_text, :]
    for k in range(1, blocks):
        grad = grad + text_in[k - 1].astype(jnp.float32)
    text_grad[...] = grad
    for copy in text_copies + image_copies + sum_copies + tg_copies + ig_copies:
        copy.wait_send()


def place(*refs):
    sem = refs[-1]
    copies = [
        pltpu.make_async_copy(refs[i], refs[i + 4], sem.at[i]) for i in (2, 3, 0, 1)
    ]
    for copy in copies:
        copy.start()
    for copy in copies:
        copy.wait()


def solution(mesh):
    lanes, blocks = mesh.shape["lane"], mesh.shape["block"]

    def body(image_rows, text_rows):
        rows, width = image_rows.shape
        images_n, texts_n = lanes * rows, blocks * rows
        group = rows * next(c for c in (4, 2, 1) if blocks % c == 0)
        groups = texts_n // group
        f32, bf16 = jnp.float32, jnp.bfloat16
        limit = 4 * (
            images_n * texts_n * 8 + (images_n + texts_n) * width * 6 + rows * width * 64
        )
        limit = min(limit, 60 * 2**20)
        sems = [pltpu.SemaphoreType.DMA((2,))]
        for count in (lanes, blocks, lanes, blocks, lanes, blocks):
            sems += [pltpu.SemaphoreType.DMA((max(count - 1, 1),))] * 2
        image_loss, text_loss, image_grad, text_grad = pl.pallas_call(
            functools.partial(kernel, lanes, blocks, group),
            out_shape=(
                jax.ShapeDtypeStruct((1, rows), f32),
                jax.ShapeDtypeStruct((1, rows), f32),
                jax.ShapeDtypeStruct((rows, width), f32),
                jax.ShapeDtypeStruct((rows, width), f32),
            ),
            in_specs=[pl.BlockSpec(memory_space=pltpu.HBM)] * 2,
            out_specs=[pl.BlockSpec(memory_space=pltpu.VMEM)] * 4,
            scratch_shapes=[
                pltpu.VMEM((rows, width), bf16),
                pltpu.VMEM((rows, width), bf16),
                pltpu.VMEM((images_n, width), bf16),
                pltpu.VMEM((texts_n, width), bf16),
                pltpu.VMEM((groups, images_n, group), f32),
                pltpu.VMEM((groups, group, images_n), f32),
                pltpu.VMEM((1, images_n), f32),
                pltpu.VMEM((max(lanes - 1, 1), 1, images_n), f32),
                pltpu.VMEM((groups, 1, group), f32),
                pltpu.VMEM((max(blocks - 1, 1), groups, 1, group), f32),
                pltpu.VMEM((images_n, width), f32),
                pltpu.VMEM((images_n, width), bf16),
                pltpu.VMEM((max(lanes - 1, 1), rows, width), bf16),
                pltpu.VMEM((texts_n, width), bf16),
                pltpu.VMEM((max(blocks - 1, 1), rows, width), bf16),
                pltpu.VMEM((texts_n, width), f32),
            ]
            + sems,
            compiler_params=pltpu.CompilerParams(
                collective_id=0, has_side_effects=True, vmem_limit_bytes=limit
            ),
        )(*(pltpu.with_memory_space_constraint(x, pltpu.HBM) for x in (image_rows, text_rows)))
        results = (image_loss, text_loss, image_grad, text_grad)
        image_loss, text_loss, image_grad, text_grad = pl.pallas_call(
            place,
            out_shape=tuple(jax.ShapeDtypeStruct(r.shape, r.dtype) for r in results),
            in_specs=[pl.BlockSpec(memory_space=pltpu.VMEM)] * 4,
            out_specs=[pl.BlockSpec(memory_space=pl.ANY)] * 4,
            scratch_shapes=[pltpu.SemaphoreType.DMA((4,))],
            compiler_params=pltpu.CompilerParams(vmem_limit_bytes=4 * rows * width * 8),
        )(*results)
        return (image_loss.reshape(rows), text_loss.reshape(rows), image_grad, text_grad)

    rows_spec = P(("unit", "block", "lane"), None)
    flat_spec = P(("unit", "block", "lane"))
    return jax.shard_map(
        body,
        mesh=mesh,
        in_specs=(rows_spec, rows_spec),
        out_specs=(flat_spec, flat_spec, rows_spec, rows_spec),
        check_vma=False,
    )
```

```python
import functools

import jax
import jax.numpy as jnp
from jax import lax
from jax.experimental import pallas as pl
from jax.experimental.pallas import tpu as pltpu
from jax.sharding import PartitionSpec as P

NT = (((1,), (1,)), ((), ()))


def unit_rows(values):
    wide = values.astype(jnp.float32)
    scale = lax.rsqrt(jnp.sum(wide * wide, axis=-1, keepdims=True) + 1e-06)
    return (wide * scale).astype(jnp.bfloat16)


def upright(row):
    return jnp.transpose(jnp.broadcast_to(row, (8, row.shape[1])))[:, :1]


def both_ways(count):
    return sorted(range(1, count), key=lambda k: (min(k, count - k), k))


def own_piece(row, pieces, mine):
    size = row.shape[1] // pieces
    return sum(
        jnp.where(mine == piece, row[:, piece * size : (piece + 1) * size], 0.0)
        for piece in range(pieces)
    )


def kernel(
    lanes,
    blocks,
    group,
    image_hbm,
    text_hbm,
    image_loss,
    text_loss,
    image_grad,
    text_grad,
    image_raw,
    text_raw,
    images,
    texts,
    power,
    power_t,
    row_mine,
    row_in,
    col_mine,
    col_in,
    image_acc,
    image_out,
    image_in,
    text_out,
    text_in,
    text_own,
    load_sem,
    send_image,
    recv_image,
    send_text,
    recv_text,
    send_row,
    recv_row,
    send_col,
    recv_col,
    send_ig,
    recv_ig,
    send_tg,
    recv_tg,
):
    lane, block = lax.axis_index("lane"), lax.axis_index("block")
    rows = image_raw.shape[0]
    images_n, texts_n = lanes * rows, blocks * rows
    groups = texts_n // group
    per_group = group // rows

    loads = [
        pltpu.make_async_copy(image_hbm, image_raw, load_sem.at[0]),
        pltpu.make_async_copy(text_hbm, text_raw, load_sem.at[1]),
    ]
    for load in loads:
        load.start()
    barrier = pltpu.get_barrier_semaphore()
    for k in range(1, blocks):
        pl.semaphore_signal(barrier, inc=1, device_id={"block": lax.rem(block + k, blocks)})
    for k in range(1, lanes):
        pl.semaphore_signal(barrier, inc=1, device_id={"lane": lax.rem(lane + k, lanes)})

    my_image = pl.ds(pl.multiple_of(lane * rows, rows), rows)
    my_text = pl.ds(pl.multiple_of(block * rows, rows), rows)
    loads[1].wait()
    texts[my_text, :] = unit_rows(text_raw[...])
    pl.semaphore_wait(barrier, lanes + blocks - 2)

    def to_block(k, src, dst, send, recv):
        return pltpu.make_async_remote_copy(
            src_ref=src,
            dst_ref=dst,
            send_sem=send.at[k - 1],
            recv_sem=recv.at[k - 1],
            device_id={"block": lax.rem(block + k, blocks)},
        )

    def to_lane(k, src, dst, send, recv):
        return pltpu.make_async_remote_copy(
            src_ref=src,
            dst_ref=dst,
            send_sem=send.at[k - 1],
            recv_sem=recv.at[k - 1],
            device_id={"lane": lax.rem(lane + k, lanes)},
        )

    text_copies = [
        to_block(k, texts.at[my_text], texts.at[my_text], send_text, recv_text)
        for k in both_ways(blocks)
    ]
    for copy in text_copies:
        copy.start()
    loads[0].wait()
    images[my_image, :] = unit_rows(image_raw[...])
    image_copies = [
        to_lane(k, images.at[my_image], images.at[my_image], send_image, recv_image)
        for k in range(1, lanes)
    ]
    for copy in image_copies:
        copy.start()

    pair = 12.0 * lax.dot_general(
        images[my_image, :], texts[my_text, :], NT, preferred_element_type=jnp.float32
    )
    eye = lax.broadcasted_iota(jnp.int32, (rows, rows), 0) == lax.broadcasted_iota(
        jnp.int32, (rows, rows), 1
    )
    matched = jnp.sum(jnp.where(eye, pair, 0.0), axis=0, keepdims=True)

    for copy in image_copies + text_copies:
        copy.wait_recv()

    def over_groups(step, start):
        if groups == 1:
            return step(0, start)
        return lax.fori_loop(0, groups, step, start)

    def group_rows(g):
        return pl.ds(g * group if groups == 1 else pl.multiple_of(g * group, group), group)

    def power_step(g, row_sum):
        some = texts[group_rows(g), :]
        p = jnp.exp(12.0 * lax.dot_general(images[...], some, NT, preferred_element_type=jnp.float32))
        q = jnp.exp(12.0 * lax.dot_general(some, images[...], NT, preferred_element_type=jnp.float32))
        power[g] = p
        power_t[g] = q
        col_mine[g] = jnp.sum(p, axis=0, keepdims=True)
        return row_sum + jnp.sum(q, axis=0, keepdims=True)

    row_mine[...] = over_groups(power_step, jnp.zeros((1, images_n), jnp.float32))
    sum_copies = [
        to_block(k, col_mine, col_in.at[k - 1], send_col, recv_col) for k in range(1, blocks)
    ] + [to_lane(k, row_mine, row_in.at[k - 1], send_row, recv_row) for k in range(1, lanes)]
    for copy in sum_copies:
        copy.start()
    for copy in sum_copies:
        copy.wait_recv()

    row_sum = row_mine[...]
    for k in range(1, lanes):
        row_sum = row_sum + row_in[k - 1]
    row_inv = 1.0 / row_sum
    row_inv_up = upright(row_inv)
    image_loss[...] = jnp.log(own_piece(row_sum, lanes, lane)) - matched

    def col_total(g):
        total = col_mine[g]
        for k in range(1, blocks):
            total = total + col_in[k - 1, g]
        return total

    def twos(shape, g, image_axis):
        ids_i = lax.broadcasted_iota(jnp.int32, shape, image_axis) - lane * rows
        ids_t = lax.broadcasted_iota(jnp.int32, shape, 1 - image_axis)
        ids_t = ids_t - (block - g * per_group) * rows
        return jnp.where((ids_t == ids_i) & (ids_i >= 0) & (ids_i < rows), 2.0, 0.0)

    def there(index, count, k):
        return pl.ds(pl.multiple_of(lax.rem(index + k, count) * rows, rows), rows)

    def text_step(g, own_col):
        total = col_total(g)
        pull_t = power_t[g] * (row_inv + upright(1.0 / total)) - twos((group, images_n), g, 1)
        part = jnp.dot(pull_t.astype(jnp.bfloat16), images[...], preferred_element_type=jnp.float32)
        text_own[group_rows(g), :] = part
        text_out[group_rows(g), :] = part.astype(jnp.bfloat16)
        return own_col + own_piece(total, per_group, block - g * per_group)

    own_col = over_groups(text_step, jnp.zeros((1, rows), jnp.float32))
    tg_copies = [
        to_block(k, text_out.at[there(block, blocks, k)], text_in.at[k - 1], send_tg, recv_tg)
        for k in range(1, blocks)
    ]
    for copy in tg_copies:
        copy.start()

    def image_part(g):
        pull = power[g] * (row_inv_up + 1.0 / col_total(g)) - twos((images_n, group), g, 0)
        return jnp.dot(
            pull.astype(jnp.bfloat16), texts[group_rows(g), :], preferred_element_type=jnp.float32
        )

    image_acc[...] = image_part(0)
    if groups > 1:

        @pl.loop(1, groups)
        def _(g):
            image_acc[...] += image_part(g)

    image_out[...] = image_acc[...].astype(jnp.bfloat16)
    ig_copies = [
        to_lane(k, image_out.at[there(lane, lanes, k)], image_in.at[k - 1], send_ig, recv_ig)
        for k in range(1, lanes)
    ]
    for copy in ig_copies:
        copy.start()
    text_loss[...] = jnp.log(own_col) - matched
    for copy in ig_copies:
        copy.wait_recv()
    grad = image_acc[my_image, :]
    for k in range(1, lanes):
        grad = grad + image_in[k - 1].astype(jnp.float32)
    image_grad[...] = grad
    for copy in tg_copies:
        copy.wait_recv()
    grad = text_own[my_text, :]
    for k in range(1, blocks):
        grad = grad + text_in[k - 1].astype(jnp.float32)
    text_grad[...] = grad
    for copy in text_copies + image_copies + sum_copies + tg_copies + ig_copies:
        copy.wait_send()


def place(*refs):
    sem = refs[-1]
    copies = [
        pltpu.make_async_copy(refs[i], refs[i + 4], sem.at[i]) for i in (2, 3, 0, 1)
    ]
    for copy in copies:
        copy.start()
    for copy in copies:
        copy.wait()


def solution(mesh):
    lanes, blocks = mesh.shape["lane"], mesh.shape["block"]

    def body(image_rows, text_rows):
        rows, width = image_rows.shape
        images_n, texts_n = lanes * rows, blocks * rows
        group = rows * next(c for c in (4, 2, 1) if blocks % c == 0)
        groups = texts_n // group
        f32, bf16 = jnp.float32, jnp.bfloat16
        limit = 4 * (
            images_n * texts_n * 8 + (images_n + texts_n) * width * 6 + rows * width * 64
        )
        limit = min(limit, 60 * 2**20)
        sems = [pltpu.SemaphoreType.DMA((2,))]
        for count in (lanes, blocks, lanes, blocks, lanes, blocks):
            sems += [pltpu.SemaphoreType.DMA((max(count - 1, 1),))] * 2
        image_loss, text_loss, image_grad, text_grad = pl.pallas_call(
            functools.partial(kernel, lanes, blocks, group),
            out_shape=(
                jax.ShapeDtypeStruct((1, rows), f32),
                jax.ShapeDtypeStruct((1, rows), f32),
                jax.ShapeDtypeStruct((rows, width), f32),
                jax.ShapeDtypeStruct((rows, width), f32),
            ),
            in_specs=[pl.BlockSpec(memory_space=pltpu.HBM)] * 2,
            out_specs=[pl.BlockSpec(memory_space=pltpu.VMEM)] * 4,
            scratch_shapes=[
                pltpu.VMEM((rows, width), bf16),
                pltpu.VMEM((rows, width), bf16),
                pltpu.VMEM((images_n, width), bf16),
                pltpu.VMEM((texts_n, width), bf16),
                pltpu.VMEM((groups, images_n, group), f32),
                pltpu.VMEM((groups, group, images_n), f32),
                pltpu.VMEM((1, images_n), f32),
                pltpu.VMEM((max(lanes - 1, 1), 1, images_n), f32),
                pltpu.VMEM((groups, 1, group), f32),
                pltpu.VMEM((max(blocks - 1, 1), groups, 1, group), f32),
                pltpu.VMEM((images_n, width), f32),
                pltpu.VMEM((images_n, width), bf16),
                pltpu.VMEM((max(lanes - 1, 1), rows, width), bf16),
                pltpu.VMEM((texts_n, width), bf16),
                pltpu.VMEM((max(blocks - 1, 1), rows, width), bf16),
                pltpu.VMEM((texts_n, width), f32),
            ]
            + sems,
            compiler_params=pltpu.CompilerParams(
                collective_id=0, has_side_effects=True, vmem_limit_bytes=limit
            ),
        )(*(pltpu.with_memory_space_constraint(x, pltpu.HBM) for x in (image_rows, text_rows)))
        results = (image_loss, text_loss, image_grad, text_grad)
        image_loss, text_loss, image_grad, text_grad = pl.pallas_call(
            place,
            out_shape=tuple(jax.ShapeDtypeStruct(r.shape, r.dtype) for r in results),
            in_specs=[pl.BlockSpec(memory_space=pltpu.VMEM)] * 4,
            out_specs=[pl.BlockSpec(memory_space=pl.ANY)] * 4,
            scratch_shapes=[pltpu.SemaphoreType.DMA((4,))],
            compiler_params=pltpu.CompilerParams(vmem_limit_bytes=4 * rows * width * 8),
        )(*results)
        return (image_loss.reshape(rows), text_loss.reshape(rows), image_grad, text_grad)

    rows_spec = P(("unit", "block", "lane"), None)
    flat_spec = P(("unit", "block", "lane"))
    return jax.shard_map(
        body,
        mesh=mesh,
        in_specs=(rows_spec, rows_spec),
        out_specs=(flat_spec, flat_spec, rows_spec, rows_spec),
        check_vma=False,
    )
```

```python
import functools

import jax
import jax.numpy as jnp
from jax import lax
from jax.experimental import pallas as pl
from jax.experimental.pallas import tpu as pltpu
from jax.sharding import PartitionSpec as P

NT = (((1,), (1,)), ((), ()))


def unit_rows(values):
    wide = values.astype(jnp.float32)
    scale = lax.rsqrt(jnp.sum(wide * wide, axis=-1, keepdims=True) + 1e-06)
    return (wide * scale).astype(jnp.bfloat16)


def upright(row):
    return jnp.transpose(jnp.broadcast_to(row, (8, row.shape[1])))[:, :1]


def both_ways(count):
    return sorted(range(1, count), key=lambda k: (min(k, count - k), k))


def own_piece(row, pieces, mine):
    size = row.shape[1] // pieces
    return sum(
        jnp.where(mine == piece, row[:, piece * size : (piece + 1) * size], 0.0)
        for piece in range(pieces)
    )


def kernel(
    lanes,
    blocks,
    group,
    image_hbm,
    text_hbm,
    image_loss,
    text_loss,
    image_grad,
    text_grad,
    image_raw,
    text_raw,
    images,
    texts,
    power,
    power_t,
    row_mine,
    row_in,
    col_mine,
    col_in,
    image_acc,
    image_out,
    image_in,
    text_out,
    text_in,
    text_own,
    load_sem,
    send_image,
    recv_image,
    send_text,
    recv_text,
    send_row,
    recv_row,
    send_col,
    recv_col,
    send_ig,
    recv_ig,
    send_tg,
    recv_tg,
):
    lane, block = lax.axis_index("lane"), lax.axis_index("block")
    rows = image_raw.shape[0]
    images_n, texts_n = lanes * rows, blocks * rows
    groups = texts_n // group
    per_group = group // rows

    loads = [
        pltpu.make_async_copy(image_hbm, image_raw, load_sem.at[0]),
        pltpu.make_async_copy(text_hbm, text_raw, load_sem.at[1]),
    ]
    for load in loads:
        load.start()
    barrier = pltpu.get_barrier_semaphore()
    for k in range(1, blocks):
        pl.semaphore_signal(barrier, inc=1, device_id={"block": lax.rem(block + k, blocks)})
    for k in range(1, lanes):
        pl.semaphore_signal(barrier, inc=1, device_id={"lane": lax.rem(lane + k, lanes)})

    my_image = pl.ds(pl.multiple_of(lane * rows, rows), rows)
    my_text = pl.ds(pl.multiple_of(block * rows, rows), rows)
    loads[1].wait()
    texts[my_text, :] = unit_rows(text_raw[...])
    pl.semaphore_wait(barrier, lanes + blocks - 2)

    def to_block(k, src, dst, send, recv):
        return pltpu.make_async_remote_copy(
            src_ref=src,
            dst_ref=dst,
            send_sem=send.at[k - 1],
            recv_sem=recv.at[k - 1],
            device_id={"block": lax.rem(block + k, blocks)},
        )

    def to_lane(k, src, dst, send, recv):
        return pltpu.make_async_remote_copy(
            src_ref=src,
            dst_ref=dst,
            send_sem=send.at[k - 1],
            recv_sem=recv.at[k - 1],
            device_id={"lane": lax.rem(lane + k, lanes)},
        )

    text_copies = [
        to_block(k, texts.at[my_text], texts.at[my_text], send_text, recv_text)
        for k in both_ways(blocks)
    ]
    for copy in text_copies:
        copy.start()
    loads[0].wait()
    images[my_image, :] = unit_rows(image_raw[...])
    image_copies = [
        to_lane(k, images.at[my_image], images.at[my_image], send_image, recv_image)
        for k in range(1, lanes)
    ]
    for copy in image_copies:
        copy.start()

    pair = 12.0 * lax.dot_general(
        images[my_image, :], texts[my_text, :], NT, preferred_element_type=jnp.float32
    )
    eye = lax.broadcasted_iota(jnp.int32, (rows, rows), 0) == lax.broadcasted_iota(
        jnp.int32, (rows, rows), 1
    )
    matched = jnp.sum(jnp.where(eye, pair, 0.0), axis=0, keepdims=True)

    for copy in image_copies + text_copies:
        copy.wait_recv()

    def over_groups(step, start):
        if groups == 1:
            return step(0, start)
        return lax.fori_loop(0, groups, step, start)

    def group_rows(g):
        return pl.ds(g * group if groups == 1 else pl.multiple_of(g * group, group), group)

    def power_step(g, row_sum):
        some = texts[group_rows(g), :]
        p = jnp.exp(12.0 * lax.dot_general(images[...], some, NT, preferred_element_type=jnp.float32))
        q = jnp.exp(12.0 * lax.dot_general(some, images[...], NT, preferred_element_type=jnp.float32))
        power[g] = p
        power_t[g] = q
        col_mine[g] = jnp.sum(p, axis=0, keepdims=True)
        return row_sum + jnp.sum(q, axis=0, keepdims=True)

    row_mine[...] = over_groups(power_step, jnp.zeros((1, images_n), jnp.float32))
    sum_copies = [
        to_block(k, col_mine, col_in.at[k - 1], send_col, recv_col) for k in range(1, blocks)
    ] + [to_lane(k, row_mine, row_in.at[k - 1], send_row, recv_row) for k in range(1, lanes)]
    for copy in sum_copies:
        copy.start()
    for copy in sum_copies:
        copy.wait_recv()

    row_sum = row_mine[...]
    for k in range(1, lanes):
        row_sum = row_sum + row_in[k - 1]
    row_inv = 1.0 / row_sum
    row_inv_up = upright(row_inv)
    image_loss[...] = jnp.log(own_piece(row_sum, lanes, lane)) - matched

    def col_total(g):
        total = col_mine[g]
        for k in range(1, blocks):
            total = total + col_in[k - 1, g]
        return total

    def twos(shape, g, image_axis):
        ids_i = lax.broadcasted_iota(jnp.int32, shape, image_axis) - lane * rows
        ids_t = lax.broadcasted_iota(jnp.int32, shape, 1 - image_axis)
        ids_t = ids_t - (block - g * per_group) * rows
        return jnp.where((ids_t == ids_i) & (ids_i >= 0) & (ids_i < rows), 2.0, 0.0)

    def there(index, count, k):
        return pl.ds(pl.multiple_of(lax.rem(index + k, count) * rows, rows), rows)

    def text_step(g, own_col):
        total = col_total(g)
        pull_t = power_t[g] * (row_inv + upright(1.0 / total)) - twos((group, images_n), g, 1)
        part = jnp.dot(pull_t.astype(jnp.bfloat16), images[...], preferred_element_type=jnp.float32)
        text_own[group_rows(g), :] = part
        text_out[group_rows(g), :] = part.astype(jnp.bfloat16)
        return own_col + own_piece(total, per_group, block - g * per_group)

    own_col = over_groups(text_step, jnp.zeros((1, rows), jnp.float32))
    tg_copies = [
        to_block(k, text_out.at[there(block, blocks, k)], text_in.at[k - 1], send_tg, recv_tg)
        for k in range(1, blocks)
    ]
    for copy in tg_copies:
        copy.start()

    def image_part(g):
        pull = power[g] * (row_inv_up + 1.0 / col_total(g)) - twos((images_n, group), g, 0)
        return jnp.dot(
            pull.astype(jnp.bfloat16), texts[group_rows(g), :], preferred_element_type=jnp.float32
        )

    image_acc[...] = image_part(0)
    if groups > 1:

        @pl.loop(1, groups)
        def _(g):
            image_acc[...] += image_part(g)

    image_out[...] = image_acc[...].astype(jnp.bfloat16)
    ig_copies = [
        to_lane(k, image_out.at[there(lane, lanes, k)], image_in.at[k - 1], send_ig, recv_ig)
        for k in range(1, lanes)
    ]
    for copy in ig_copies:
        copy.start()
    text_loss[...] = jnp.log(own_col) - matched
    for copy in ig_copies:
        copy.wait_recv()
    grad = image_acc[my_image, :]
    for k in range(1, lanes):
        grad = grad + image_in[k - 1].astype(jnp.float32)
    image_grad[...] = grad
    for copy in text_copies + image_copies + sum_copies + ig_copies:
        copy.wait_send()
    for copy in tg_copies:
        copy.wait_recv()
    grad = text_own[my_text, :]
    for k in range(1, blocks):
        grad = grad + text_in[k - 1].astype(jnp.float32)
    text_grad[...] = grad
    for copy in tg_copies:
        copy.wait_send()


def place(*refs):
    sem = refs[-1]
    copies = [
        pltpu.make_async_copy(refs[i], refs[i + 4], sem.at[i]) for i in (2, 3, 0, 1)
    ]
    for copy in copies:
        copy.start()
    for copy in copies:
        copy.wait()


def solution(mesh):
    lanes, blocks = mesh.shape["lane"], mesh.shape["block"]

    def body(image_rows, text_rows):
        rows, width = image_rows.shape
        images_n, texts_n = lanes * rows, blocks * rows
        group = rows * next(c for c in (4, 2, 1) if blocks % c == 0)
        groups = texts_n // group
        f32, bf16 = jnp.float32, jnp.bfloat16
        limit = 4 * (
            images_n * texts_n * 8 + (images_n + texts_n) * width * 6 + rows * width * 64
        )
        limit = min(limit, 60 * 2**20)
        sems = [pltpu.SemaphoreType.DMA((2,))]
        for count in (lanes, blocks, lanes, blocks, lanes, blocks):
            sems += [pltpu.SemaphoreType.DMA((max(count - 1, 1),))] * 2
        image_loss, text_loss, image_grad, text_grad = pl.pallas_call(
            functools.partial(kernel, lanes, blocks, group),
            out_shape=(
                jax.ShapeDtypeStruct((1, rows), f32),
                jax.ShapeDtypeStruct((1, rows), f32),
                jax.ShapeDtypeStruct((rows, width), f32),
                jax.ShapeDtypeStruct((rows, width), f32),
            ),
            in_specs=[pl.BlockSpec(memory_space=pltpu.HBM)] * 2,
            out_specs=[pl.BlockSpec(memory_space=pltpu.VMEM)] * 4,
            scratch_shapes=[
                pltpu.VMEM((rows, width), bf16),
                pltpu.VMEM((rows, width), bf16),
                pltpu.VMEM((images_n, width), bf16),
                pltpu.VMEM((texts_n, width), bf16),
                pltpu.VMEM((groups, images_n, group), f32),
                pltpu.VMEM((groups, group, images_n), f32),
                pltpu.VMEM((1, images_n), f32),
                pltpu.VMEM((max(lanes - 1, 1), 1, images_n), f32),
                pltpu.VMEM((groups, 1, group), f32),
                pltpu.VMEM((max(blocks - 1, 1), groups, 1, group), f32),
                pltpu.VMEM((images_n, width), f32),
                pltpu.VMEM((images_n, width), bf16),
                pltpu.VMEM((max(lanes - 1, 1), rows, width), bf16),
                pltpu.VMEM((texts_n, width), bf16),
                pltpu.VMEM((max(blocks - 1, 1), rows, width), bf16),
                pltpu.VMEM((texts_n, width), f32),
            ]
            + sems,
            compiler_params=pltpu.CompilerParams(
                collective_id=0, has_side_effects=True, vmem_limit_bytes=limit
            ),
        )(*(pltpu.with_memory_space_constraint(x, pltpu.HBM) for x in (image_rows, text_rows)))
        results = (image_loss, text_loss, image_grad, text_grad)
        image_loss, text_loss, image_grad, text_grad = pl.pallas_call(
            place,
            out_shape=tuple(jax.ShapeDtypeStruct(r.shape, r.dtype) for r in results),
            in_specs=[pl.BlockSpec(memory_space=pltpu.VMEM)] * 4,
            out_specs=[pl.BlockSpec(memory_space=pl.ANY)] * 4,
            scratch_shapes=[pltpu.SemaphoreType.DMA((4,))],
            compiler_params=pltpu.CompilerParams(vmem_limit_bytes=4 * rows * width * 8),
        )(*results)
        return (image_loss.reshape(rows), text_loss.reshape(rows), image_grad, text_grad)

    rows_spec = P(("unit", "block", "lane"), None)
    flat_spec = P(("unit", "block", "lane"))
    return jax.shard_map(
        body,
        mesh=mesh,
        in_specs=(rows_spec, rows_spec),
        out_specs=(flat_spec, flat_spec, rows_spec, rows_spec),
        check_vma=False,
    )
```
